256 devices in a mesh: grp: 2 (over y), lon: 64 (over x, z), lat: 2 (over core).
Axes of the slice: x: 4, y: 2, z: 16, core: 2. Of those that a mesh axis runs over, the one named last changes fastest.
The devices are a block of a 4x16x16 slice.
Arguments:
- surface_field: bfloat16 [512, 512, 256], P(('grp', 'lat'), 'lon'), parts along dimension 0, may hold values from -6 to 6
- conv_a: bfloat16 [3, 3, 256, 512], replicated, may hold values from -0.125 to 0.125
- conv_b: bfloat16 [3, 3, 512, 512], replicated, may hold values from -0.09375 to 0.09375
- norm_gain: float32 [512], replicated, may hold values from 0.1 to 1.9
- qkv_weight: bfloat16 [512, 3072], replicated, may hold values from -3 to 3, as said below
- out_weight: bfloat16 [1024, 512], replicated, may hold values from -0.1875 to 0.1875
Outputs:
- mixed_out: bfloat16 [128, 128, 512], P(('grp', 'lat'), 'lon'), parts along dimension 0
The draws below stay inside these ranges and needn't reach their ends.
There are 2 independent parts, one for each index of `grp`. The reference program is written for one: setup_inputs(seed, part) draws one part's arguments, and reference() takes and returns one part's arrays. A program takes and returns all parts, laid end to end along the dimension named above; an argument that names none is the same for every part. Nothing has to cross between parts.
Inputs may be any that keep to these rules, and one draw needn't show every extreme that they name: `qkv_weight`: columns hold queries, keys and values in that order, each 16 heads of 64 entries.
All inputs are finite; a program needn't handle non-finite values.
Results may differ from the reference program's by a relative error of at most 0.012.
The reference program's roundings to bfloat16 on the way (of `pooled_first`, `normed`, `projected`, `weights` and `attended`) count: a program that leaves them out, or rounds other values in their place, can miss the bound.
Values may be sent and summed in bfloat16 or wider, within the bound.
No kernel may reach another device: no remote copies, remote signals or barrier semaphores. Data moves between devices by JAX's collectives and lax.ppermute only.
A program may use at most 128 MiB of HBM per device.

```python
import math
import jax
import jax.numpy as jnp
from jax import lax

CA = 256
CB = 512
HEADS = 16
HEAD_DIM = 64
WIDTH = 1024
HA = 256
WA = 512


def draw_qkv_weight(key, part):
    key_query = jax.random.fold_in(key, 0)
    fan_scale = CB ** (-0.5)
    drawn = jnp.clip(jax.random.normal(key_query, (CB, 3 * HEADS * HEAD_DIM), jnp.float32) * 1.7, -6.0, 6.0) * fan_scale
    return drawn.astype(jnp.bfloat16)


def levels(rng, dims, cuts, low, top_value):
    def one(position, shards_of):
        draws = jax.random.uniform(jax.random.fold_in(jax.random.fold_in(rng, 6), position), (shards_of,), jnp.float32, low / len(cuts), top_value / len(cuts))
        return jnp.repeat(jnp.exp(draws), dims[position] // shards_of).reshape((-1,) + (1,) * (len(dims) - position - 1))

    loudness = one(*cuts[0])
    for cut in cuts[1:]:
        loudness = loudness * one(*cut)
    return loudness


def bell_draw(key, dims, scale, most, pieces=(), held_as=jnp.bfloat16):
    factor_of = levels(key, dims, pieces, -0.22, 0.18) if pieces else 1.0
    values = jax.random.normal(key, dims, jnp.float32) * scale * factor_of
    return jnp.minimum(jnp.maximum(values, -most), most).astype(held_as)


def setup_inputs(seed: int = 0, part: int = 0) -> dict:
    keys = jax.random.split(jax.random.key(seed), 7)
    part_keys = jax.random.split(jax.random.fold_in(keys[6], part), 7)
    surface_field = bell_draw(part_keys[0], (HA, WA, CA), 1.0, 6.0, ((0, 2), (1, 64)))
    conv_a = bell_draw(keys[1], (3, 3, CA, CB), (9 * CA) ** -0.5, 0.125)
    conv_b = bell_draw(keys[2], (3, 3, CB, CB), (9 * CB) ** -0.5, 0.09375)
    norm_gain = jnp.clip(1.0 + 0.18 * jax.random.normal(keys[3], (CB,), jnp.float32), 0.1, 1.9)
    qkv_weight = draw_qkv_weight(jax.random.fold_in(keys[6], 71), part)
    out_weight = bell_draw(keys[5], (WIDTH, CB), WIDTH ** -0.5, 0.1875)
    return dict(surface_field=surface_field, conv_a=conv_a, conv_b=conv_b, norm_gain=norm_gain, qkv_weight=qkv_weight, out_weight=out_weight)


def convolve(values_in, weight):
    beside_all = jnp.pad(values_in, ((0, 0), (1, 1), (0, 0)), mode='wrap')
    beside_all = jnp.pad(beside_all, ((1, 1), (0, 0), (0, 0)))
    return lax.conv_general_dilated(beside_all[None], weight, (1, 1), 'VALID', dimension_numbers=('NHWC', 'HWIO', 'NHWC'), preferred_element_type=jnp.float32)[0]

def average_pool(values_in):
    rows_in, cols_in, chans_in = values_in.shape
    return values_in.reshape(rows_in // 2, 2, cols_in // 2, 2, chans_in).mean(axis=(1, 3))

def layer_norm(tokens_flat, norm_gain):
    centred = tokens_flat - lax.optimization_barrier(jnp.mean(tokens_flat, axis=-1, keepdims=True))
    spread = lax.optimization_barrier(jnp.mean(centred * centred, axis=-1, keepdims=True))
    return centred * lax.rsqrt(spread + 0.01) * norm_gain

def softmax_rows(scores):
    maxima = lax.optimization_barrier(jnp.max(scores, axis=-1, keepdims=True))
    raised = jnp.exp(scores - maxima)
    return raised / lax.optimization_barrier(jnp.sum(raised, axis=-1, keepdims=True))

def reference(surface_field, conv_a, conv_b, norm_gain, qkv_weight, out_weight):
    first_out = jax.nn.silu(convolve(surface_field, conv_a))
    pooled_first = average_pool(first_out).astype(jnp.bfloat16)
    second_out = jax.nn.silu(convolve(pooled_first, conv_b))
    pooled_second = average_pool(second_out)
    rows_out, cols_out = (pooled_second.shape[0], pooled_second.shape[1])
    token_count = rows_out * cols_out
    tokens_flat = pooled_second.reshape(token_count, CB)
    normed = layer_norm(tokens_flat, norm_gain).astype(jnp.bfloat16)
    projected = jnp.dot(normed, qkv_weight, preferred_element_type=jnp.float32).astype(jnp.bfloat16)
    per_head = projected.reshape(token_count, 3, HEADS, HEAD_DIM).transpose(1, 2, 0, 3)
    block_rows = math.gcd(token_count, 512)
    score_scale = HEAD_DIM ** (-0.5)

    def one_head(triple):
        queries, keys_here, values_here = triple

        def one_block(query_block):
            scores = jnp.dot(query_block, keys_here.T, preferred_element_type=jnp.float32) * score_scale
            weights = softmax_rows(scores).astype(jnp.bfloat16)
            return jnp.dot(weights, values_here, preferred_element_type=jnp.float32).astype(jnp.bfloat16)
        blocks = lax.map(one_block, queries.reshape(token_count // block_rows, block_rows, HEAD_DIM))
        return blocks.reshape(token_count, HEAD_DIM)
    attended = lax.map(one_head, (per_head[0], per_head[1], per_head[2]))
    attended = attended.transpose(1, 0, 2).reshape(token_count, HEADS * HEAD_DIM)
    mixed_out = tokens_flat + jnp.dot(attended, out_weight, preferred_element_type=jnp.float32)
    return mixed_out.reshape(rows_out, cols_out, CB).astype(jnp.bfloat16)
```

```python
import functools
import math

import jax
import jax.numpy as jnp
from jax import lax
from jax.experimental import pallas as pl
from jax.experimental.pallas import tpu as pltpu
from jax.sharding import PartitionSpec as P

CB = 512
HEADS = 16
HEAD_DIM = 64
REACH = 3
BF = jnp.bfloat16
F32 = jnp.float32
VMEM = pl.BlockSpec(memory_space=pltpu.VMEM)
SMEM = pl.BlockSpec(memory_space=pltpu.SMEM)
HBM = pl.BlockSpec(memory_space=pltpu.HBM)


def silu(v):
    half = 0.5 * v
    return half + half * jnp.tanh(half)


def lanes_of(shape):
    return lax.broadcasted_iota(jnp.int32, shape, len(shape) - 1)


def conv_kernel(
    lat_ref, mid_ref, low_ref, high_ref, lat_mid_ref, lat_low_ref, lat_high_ref, gain_ref,
    conv_a_hbm, conv_b_hbm, qkv_hbm,
    tok_ref, out_ref,
    conv_a_ref, conv_b_ref, qkv_ref, wide, shifted, pool_a, ready, pool_b, sems,
):
    copies = [
        pltpu.make_async_copy(conv_a_hbm, conv_a_ref, sems.at[0]),
        pltpu.make_async_copy(conv_b_hbm, conv_b_ref, sems.at[1]),
        pltpu.make_async_copy(qkv_hbm, qkv_ref, sems.at[2]),
    ]
    for copy in copies:
        copy.start()
    lat = lat_ref[0]
    last = lat_ref[1] - 1
    cols, rows, chans = mid_ref.shape
    span = shifted.shape[2]
    for ref, edge, at in (
        (low_ref, lat_low_ref, 0),
        (mid_ref, lat_mid_ref, REACH),
        (high_ref, lat_high_ref, REACH + cols),
    ):
        n = ref.shape[0]
        wide[at : at + n, REACH : REACH + rows, :] = ref[...].astype(F32)
        rows_edge = edge[...].astype(F32)
        nothing = jnp.zeros_like(rows_edge)
        wide[at : at + n, 0:REACH, :] = jnp.where(lat == 0, nothing, rows_edge)
        wide[at : at + n, REACH + rows : 2 * REACH + rows, :] = jnp.where(
            lat == last, nothing, rows_edge
        )
    tail = 2 * REACH + rows
    wide[:, tail:, :] = jnp.zeros((wide.shape[0], wide.shape[1] - tail, chans), F32)
    for a in range(3):
        shifted[a] = wide[:, a : a + span, :].astype(BF)
    copies[0].wait()
    slabs = CB // 128
    pooled_cols = cols // 2 + 2
    for c in range(pooled_cols):
        parts = [
            shifted[a, 2 * c + b : 2 * c + b + 2].reshape(2 * span, chans)
            for a in range(3)
            for b in range(3)
        ]
        first = silu(
            jnp.dot(jnp.concatenate(parts, axis=1), conv_a_ref[...], preferred_element_type=F32)
        )
        pair = first[:span] + first[span:]
        for s in range(slabs):
            pool_a[c * slabs + s] = pair[:, 128 * s : 128 * (s + 1)]
    pooled_rows = rows // 2

    @pl.when(lat == 0)
    def _():
        pool_a[:, 0:2, :] = jnp.zeros((pool_a.shape[0], 2, 128), F32)

    @pl.when(lat == last)
    def _():
        pool_a[:, rows + 2 : rows + 4, :] = jnp.zeros((pool_a.shape[0], 2, 128), F32)

    for c in range(pooled_cols):
        for s in range(slabs):
            for a in range(3):
                even = pool_a[c * slabs + s, pl.ds(2 * a, pooled_rows, stride=2), :]
                odd = pool_a[c * slabs + s, pl.ds(2 * a + 1, pooled_rows, stride=2), :]
                ready[a, c, :, 128 * s : 128 * (s + 1)] = ((even + odd) * 0.25).astype(BF)
    copies[1].wait()
    cols_b = cols // 2
    parts = [
        ready[a, b : b + cols_b].reshape(cols_b * pooled_rows, CB)
        for a in range(3)
        for b in range(3)
    ]
    second = silu(
        jnp.dot(jnp.concatenate(parts, axis=1), conv_b_ref[...], preferred_element_type=F32)
    )
    tokens = []
    for c in range(cols_b // 2):
        at = 2 * c * pooled_rows
        pair = second[at : at + pooled_rows] + second[at + pooled_rows : at + 2 * pooled_rows]
        pieces = []
        for s in range(slabs):
            pool_b[c * slabs + s] = pair[:, 128 * s : 128 * (s + 1)]
            even = pool_b[c * slabs + s, pl.ds(0, pooled_rows // 2, stride=2), :]
            odd = pool_b[c * slabs + s, pl.ds(1, pooled_rows // 2, stride=2), :]
            pieces.append((even + odd) * 0.25)
        tokens.append(jnp.concatenate(pieces, axis=1))
    tokens = jnp.concatenate(tokens, axis=0)
    tok_ref[...] = tokens
    centred = tokens - jnp.mean(tokens, axis=-1, keepdims=True)
    spread = jnp.mean(centred * centred, axis=-1, keepdims=True)
    normed = (centred * lax.rsqrt(spread + 0.01) * gain_ref[...]).astype(BF)
    copies[2].wait()
    width = HEADS * HEAD_DIM
    count = tokens.shape[0]
    half = count // 2
    projected = jnp.dot(normed, qkv_ref[...], preferred_element_type=F32)
    below = lanes_of((count, 128)) < HEAD_DIM
    below_half = lanes_of((half, 128)) < HEAD_DIM
    for pair in range(HEADS // 2):
        q, k, v = (
            projected[:, width * s + 128 * pair : width * s + 128 * (pair + 1)] for s in range(3)
        )
        turned = [pltpu.roll(x, HEAD_DIM, 1) for x in (q, k, v)]
        h = 2 * pair
        out_ref[h, :count] = jnp.where(below, k, turned[2]).astype(BF)
        out_ref[h + 1, :count] = jnp.where(below, turned[1], v).astype(BF)
        out_ref[h, count:] = jnp.where(below_half, q[:half], turned[0][half:]).astype(BF)
        out_ref[h + 1, count:] = jnp.where(below_half, turned[0][:half], q[half:]).astype(BF)


def attention_kernel(q_ref, *refs):
    kv_refs, (out_ref, queries, ones_vals) = refs[:-3], refs[-3:]
    packed_rows = q_ref.shape[0]
    keys = kv_refs[0].shape[0]
    packed = q_ref[...].astype(F32)
    below = lanes_of((packed_rows, 128)) < HEAD_DIM
    zero = jnp.zeros_like(packed)
    queries[0] = jnp.where(below, packed, zero).astype(BF)
    queries[1] = jnp.where(below, pltpu.roll(packed, HEAD_DIM, 1), zero).astype(BF)
    one = jnp.ones((keys, 128), BF)
    below_keys = lanes_of((keys, 128)) < HEAD_DIM
    for i, kv in enumerate(kv_refs):
        ones_vals[i] = jnp.where(below_keys, one, kv[...])
    factor = HEAD_DIM ** (-0.5) * math.log2(math.e)
    block = 128

    def step(j, carry):
        at = pl.multiple_of(j * block, block)
        q = queries[:, pl.ds(at, block), :].reshape(2 * block, 128)
        top = jnp.full((2 * block, 1), -jnp.inf, F32)
        acc = jnp.zeros((2 * block, 128), F32)
        for i, kv in enumerate(kv_refs):
            scores = lax.dot_general(
                q, kv[...], (((1,), (1,)), ((), ())), preferred_element_type=F32
            )
            new_top = jnp.maximum(top, jnp.max(scores, axis=-1, keepdims=True))
            raised = jnp.exp2((scores - new_top) * factor).astype(BF)
            part = jnp.dot(raised, ones_vals[i], preferred_element_type=F32)
            acc = part if i == 0 else acc * jnp.exp2((top - new_top) * factor) + part
            top = new_top
        turned = pltpu.roll(acc, HEAD_DIM, 1)
        low = turned[:block] / acc[:block]
        high = acc[block:] / turned[block:]
        mask = lanes_of((block, 128)) < HEAD_DIM
        out_ref[pl.ds(at, block), :] = jnp.where(mask, low, high).astype(BF)
        return carry

    lax.fori_loop(0, packed_rows // block, step, 0)


def out_kernel(back_ref, tok_ref, weight_ref, out_ref):
    half = back_ref.shape[1]
    low, high = [], []
    mask = lanes_of((half, 128)) < HEAD_DIM
    for pair in range(HEADS // 2):
        even = back_ref[2 * pair].astype(F32)
        odd = back_ref[2 * pair + 1].astype(F32)
        low.append(jnp.where(mask, even, pltpu.roll(odd, HEAD_DIM, 1)).astype(BF))
        high.append(jnp.where(mask, pltpu.roll(even, HEAD_DIM, 1), odd).astype(BF))
    attended = jnp.concatenate(
        [jnp.concatenate(low, axis=1), jnp.concatenate(high, axis=1)], axis=0
    )
    mixed = tok_ref[...] + jnp.dot(attended, weight_ref[...], preferred_element_type=F32)
    out_ref[...] = mixed.astype(BF)


def body(surface_field, conv_a, conv_b, norm_gain, qkv_weight, out_weight):
    lon_count = lax.axis_size("lon")
    lat_count = lax.axis_size("lat")
    lat = lax.axis_index("lat")
    rows, cols, chans = surface_field.shape
    field = surface_field.transpose(1, 0, 2)
    forward = [(i, (i + 1) % lon_count) for i in range(lon_count)]
    backward = [(target, source) for source, target in forward]

    def across(pairs):
        return [
            (s * lat_count + c, t * lat_count + (c + 1) % lat_count)
            for s, t in pairs
            for c in range(lat_count)
        ]

    swap = [(c, (c + 1) % lat_count) for c in range(lat_count)]
    edge = jnp.where(lat == 0, field[:, rows - REACH :], field[:, :REACH])
    low = lax.ppermute(field[cols - REACH :], "lon", forward)
    high = lax.ppermute(field[:REACH], "lon", backward)
    lat_mid = lax.ppermute(edge, "lat", swap)
    lat_low = lax.ppermute(edge[cols - REACH :], ("lon", "lat"), across(forward))
    lat_high = lax.ppermute(edge[:REACH], ("lon", "lat"), across(backward))

    wide_cols = cols + 2 * REACH
    span = -(-(rows + 4) // 16) * 16
    pooled_cols = cols // 2 + 2
    pooled_rows = rows // 2
    count = (rows // 4) * (cols // 4)
    half = count // 2
    slabs = CB // 128
    where = jnp.stack([lat, jnp.int32(lat_count)]).astype(jnp.int32)
    tokens, outgoing = pl.pallas_call(
        conv_kernel,
        out_shape=(
            jax.ShapeDtypeStruct((count, CB), F32),
            jax.ShapeDtypeStruct((HEADS, count + half, 128), BF),
        ),
        in_specs=[SMEM] + [VMEM] * 7 + [HBM] * 3,
        out_specs=(VMEM, VMEM),
        scratch_shapes=[
            pltpu.VMEM((9 * chans, CB), BF),
            pltpu.VMEM((9 * CB, CB), BF),
            pltpu.VMEM(qkv_weight.shape, BF),
            pltpu.VMEM((wide_cols, span + 8, chans), F32),
            pltpu.VMEM((3, wide_cols, span, chans), BF),
            pltpu.VMEM((pooled_cols * slabs, span, 128), F32),
            pltpu.VMEM((3, pooled_cols, pooled_rows, CB), BF),
            pltpu.VMEM((cols // 4 * slabs, pooled_rows, 128), F32),
            pltpu.SemaphoreType.DMA((3,)),
        ],
        compiler_params=pltpu.CompilerParams(vmem_limit_bytes=40 * 2**20),
        name="convs",
    )(
        where, field, low, high, lat_mid, lat_low, lat_high, norm_gain.reshape(1, CB),
        conv_a.reshape(9 * chans, CB), conv_b.reshape(9 * CB, CB), qkv_weight,
    )

    residues = lon_count // HEADS
    groups = [[r * HEADS + h for h in range(HEADS)] for r in range(residues)]
    arrived = lax.all_to_all(outgoing, "lon", 0, 0, axis_index_groups=groups, tiled=True)
    queries = arrived[:, count:].reshape(HEADS * half, 128)
    own = arrived[:, :count].reshape(HEADS * count, 128)
    pieces = [own]
    for d in range(1, residues):
        pairs = [
            (r * HEADS + h, (r + d) % residues * HEADS + h)
            for r in range(residues)
            for h in range(HEADS)
        ]
        pieces.append(lax.ppermute(own, "lon", pairs))
    pieces += [lax.ppermute(piece, "lat", swap) for piece in pieces]
    attended = pl.pallas_call(
        attention_kernel,
        out_shape=jax.ShapeDtypeStruct((HEADS * half, 128), BF),
        in_specs=[VMEM] * (1 + len(pieces)),
        out_specs=VMEM,
        scratch_shapes=[
            pltpu.VMEM((2, HEADS * half, 128), BF),
            pltpu.VMEM((len(pieces), HEADS * count, 128), BF),
        ],
        compiler_params=pltpu.CompilerParams(vmem_limit_bytes=40 * 2**20),
        name="attention",
    )(queries, *pieces)
    returned = lax.all_to_all(
        attended.reshape(HEADS, half, 128), "lon", 0, 0, axis_index_groups=groups, tiled=True
    )
    mixed = pl.pallas_call(
        out_kernel,
        out_shape=jax.ShapeDtypeStruct((count, CB), BF),
        in_specs=[VMEM] * 3,
        out_specs=VMEM,
        name="mix",
    )(returned, tokens, out_weight)
    return mixed.reshape(cols // 4, rows // 4, CB).transpose(1, 0, 2)


def solution(mesh):
    in_specs = (P(("grp", "lat"), "lon", None), P(), P(), P(), P(), P())
    out_specs = P(("grp", "lat"), "lon", None)
    return jax.shard_map(body, mesh=mesh, in_specs=in_specs, out_specs=out_specs, check_vma=False)
```

```python
import functools
import math

import jax
import jax.numpy as jnp
from jax import lax
from jax.experimental import pallas as pl
from jax.experimental.pallas import tpu as pltpu
from jax.sharding import PartitionSpec as P

CB = 512
HEADS = 16
HEAD_DIM = 64
REACH = 3
PIECES = 2
BF = jnp.bfloat16
F32 = jnp.float32
VMEM = pl.BlockSpec(memory_space=pltpu.VMEM)
SMEM = pl.BlockSpec(memory_space=pltpu.SMEM)
HBM = pl.BlockSpec(memory_space=pltpu.HBM)


def silu(v):
    half = 0.5 * v
    return half + half * jnp.tanh(half)


def lanes_of(shape):
    return lax.broadcasted_iota(jnp.int32, shape, len(shape) - 1)


def conv_kernel(
    lat_ref, mid_ref, low_ref, high_ref, edge_ref, gain_ref,
    conv_a_hbm, conv_b_hbm, qkv_hbm,
    tok_ref, out_ref,
    conv_a_ref, conv_b_ref, qkv_ref, wide, shifted, pool_a, ready, pool_b, sems,
):
    copies = [
        pltpu.make_async_copy(conv_a_hbm, conv_a_ref, sems.at[0]),
        pltpu.make_async_copy(conv_b_hbm, conv_b_ref, sems.at[1]),
        pltpu.make_async_copy(qkv_hbm, qkv_ref, sems.at[2]),
    ]
    for copy in copies:
        copy.start()
    lat = lat_ref[0]
    last = lat_ref[1] - 1
    cols, rows, chans = mid_ref.shape
    span = shifted.shape[2]
    for ref, edge_rows, at in (
        (low_ref, low_ref[:, rows:], 0),
        (mid_ref, edge_ref[...], REACH),
        (high_ref, high_ref[:, rows:], REACH + cols),
    ):
        n = ref.shape[0]
        wide[at : at + n, REACH : REACH + rows, :] = ref[:, :rows].astype(F32)
        rows_edge = edge_rows.astype(F32)
        nothing = jnp.zeros_like(rows_edge)
        wide[at : at + n, 0:REACH, :] = jnp.where(lat == 0, nothing, rows_edge)
        wide[at : at + n, REACH + rows : 2 * REACH + rows, :] = jnp.where(
            lat == last, nothing, rows_edge
        )
    tail = 2 * REACH + rows
    wide[:, tail:, :] = jnp.zeros((wide.shape[0], wide.shape[1] - tail, chans), F32)
    for a in range(3):
        shifted[a] = wide[:, a : a + span, :].astype(BF)
    copies[0].wait()
    slabs = CB // 128
    pooled_cols = cols // 2 + 2
    for c in range(pooled_cols):
        parts = [
            shifted[a, 2 * c + b : 2 * c + b + 2].reshape(2 * span, chans)
            for a in range(3)
            for b in range(3)
        ]
        first = silu(
            jnp.dot(jnp.concatenate(parts, axis=1), conv_a_ref[...], preferred_element_type=F32)
        )
        pair = first[:span] + first[span:]
        for s in range(slabs):
            pool_a[c * slabs + s] = pair[:, 128 * s : 128 * (s + 1)]
    pooled_rows = rows // 2

    @pl.when(lat == 0)
    def _():
        pool_a[:, 0:2, :] = jnp.zeros((pool_a.shape[0], 2, 128), F32)

    @pl.when(lat == last)
    def _():
        pool_a[:, rows + 2 : rows + 4, :] = jnp.zeros((pool_a.shape[0], 2, 128), F32)

    for c in range(pooled_cols):
        for s in range(slabs):
            for a in range(3):
                even = pool_a[c * slabs + s, pl.ds(2 * a, pooled_rows, stride=2), :]
                odd = pool_a[c * slabs + s, pl.ds(2 * a + 1, pooled_rows, stride=2), :]
                ready[a, c, :, 128 * s : 128 * (s + 1)] = ((even + odd) * 0.25).astype(BF)
    copies[1].wait()
    cols_b = cols // 2
    parts = [
        ready[a, b : b + cols_b].reshape(cols_b * pooled_rows, CB)
        for a in range(3)
        for b in range(3)
    ]
    second = silu(
        jnp.dot(jnp.concatenate(parts, axis=1), conv_b_ref[...], preferred_element_type=F32)
    )
    tokens = []
    for c in range(cols_b // 2):
        at = 2 * c * pooled_rows
        pair = second[at : at + pooled_rows] + second[at + pooled_rows : at + 2 * pooled_rows]
        pieces = []
        for s in range(slabs):
            pool_b[c * slabs + s] = pair[:, 128 * s : 128 * (s + 1)]
            even = pool_b[c * slabs + s, pl.ds(0, pooled_rows // 2, stride=2), :]
            odd = pool_b[c * slabs + s, pl.ds(1, pooled_rows // 2, stride=2), :]
            pieces.append((even + odd) * 0.25)
        tokens.append(jnp.concatenate(pieces, axis=1))
    tokens = jnp.concatenate(tokens, axis=0)
    tok_ref[...] = tokens
    centred = tokens - jnp.mean(tokens, axis=-1, keepdims=True)
    spread = jnp.mean(centred * centred, axis=-1, keepdims=True)
    normed = (centred * lax.rsqrt(spread + 0.01) * gain_ref[...]).astype(BF)
    copies[2].wait()
    width = HEADS * HEAD_DIM
    count = tokens.shape[0]
    half = count // 2
    projected = jnp.dot(normed, qkv_ref[...], preferred_element_type=F32)
    below = lanes_of((count, 128)) < HEAD_DIM
    below_half = lanes_of((half, 128)) < HEAD_DIM
    for pair in range(HEADS // 2):
        q, k, v = (
            projected[:, width * s + 128 * pair : width * s + 128 * (pair + 1)] for s in range(3)
        )
        turned = [pltpu.roll(x, HEAD_DIM, 1) for x in (q, k, v)]
        h = 2 * pair
        out_ref[h, :count] = jnp.where(below, k, turned[2]).astype(BF)
        out_ref[h + 1, :count] = jnp.where(below, turned[1], v).astype(BF)
        out_ref[h, count:] = jnp.where(below_half, q[:half], turned[0][half:]).astype(BF)
        out_ref[h + 1, count:] = jnp.where(below_half, turned[0][:half], q[half:]).astype(BF)


def attention_kernel(first, final, *refs):
    refs = list(refs)
    q_ref = refs.pop(0)
    kv_refs = [refs.pop(0) for _ in range(PIECES)]
    held = None if first else (refs.pop(0), refs.pop(0))
    ones_vals = refs.pop()
    queries, acc_ref, top_ref = (None, None, None) if final else refs if first else (None, *refs)
    keys = kv_refs[0].shape[0]
    mask_keys = lanes_of((keys, 128)) < HEAD_DIM
    if first:
        rows = q_ref.shape[0]
        packed = q_ref[...].astype(F32)
        below = lanes_of((rows, 128)) < HEAD_DIM
        zero = jnp.zeros_like(packed)
        queries[0] = jnp.where(below, packed, zero).astype(BF)
        queries[1] = jnp.where(below, pltpu.roll(packed, HEAD_DIM, 1), zero).astype(BF)
    else:
        queries = q_ref
        rows = q_ref.shape[1]
    one = jnp.ones((keys, 128), BF)
    for i, kv in enumerate(kv_refs):
        ones_vals[i] = jnp.where(mask_keys, one, kv[...])
    factor = HEAD_DIM ** (-0.5) * math.log2(math.e)
    block = rows // 2
    units = [(at, i) for at in range(0, rows, block) for i in range(PIECES)]

    def score(unit):
        at, i = unit
        return lax.dot_general(
            queries[:, at : at + block, :].reshape(2 * block, 128),
            kv_refs[i][...],
            (((1,), (1,)), ((), ())),
            preferred_element_type=F32,
        )

    ahead = score(units[0])
    for n, (at, i) in enumerate(units):
        scores = ahead
        if n + 1 < len(units):
            ahead = score(units[n + 1])
        if i == 0:
            if first:
                top = jnp.full((2 * block, 1), -jnp.inf, F32)
                acc = None
            else:
                top = held[1][:, at : at + block, :].reshape(2 * block, 128)[:, :1]
                acc = held[0][:, at : at + block, :].reshape(2 * block, 128)
        new_top = jnp.maximum(top, jnp.max(scores, axis=-1, keepdims=True))
        raised = jnp.exp2((scores - new_top) * factor).astype(BF)
        part = jnp.dot(raised, ones_vals[i], preferred_element_type=F32)
        acc = part if acc is None else acc * jnp.exp2((top - new_top) * factor) + part
        top = new_top
        if i < PIECES - 1:
            continue
        if not final:
            acc_ref[:, at : at + block, :] = acc.reshape(2, block, 128)
            wide = jnp.broadcast_to(top, (2 * block, 128))
            top_ref[:, at : at + block, :] = wide.reshape(2, block, 128)
            continue
        turned = pltpu.roll(acc, HEAD_DIM, 1)
        low = turned[:block] / acc[:block]
        high = acc[block:] / turned[block:]
        mask = lanes_of((block, 128)) < HEAD_DIM
        refs[0][at : at + block, :] = jnp.where(mask, low, high).astype(BF)


def attend(queries, pieces, held, final):
    first = held is None
    rows = queries.shape[0] if first else queries.shape[1]
    keys = pieces[0].shape[0]
    state = [jax.ShapeDtypeStruct((2, rows, 128), F32)] * 2
    if final:
        outs = jax.ShapeDtypeStruct((rows, 128), BF)
    else:
        outs = tuple(([jax.ShapeDtypeStruct((2, rows, 128), BF)] if first else []) + state)
    return pl.pallas_call(
        functools.partial(attention_kernel, first, final),
        out_shape=outs,
        in_specs=[VMEM] * (1 + PIECES + (0 if first else 2)),
        out_specs=VMEM if final else (VMEM,) * len(outs),
        scratch_shapes=[pltpu.VMEM((PIECES, keys, 128), BF)],
        compiler_params=pltpu.CompilerParams(vmem_limit_bytes=24 * 2**20),
        cost_estimate=pl.CostEstimate(
            flops=4 * 2 * rows * PIECES * keys * 256,
            transcendentals=2 * rows * PIECES * keys,
            bytes_accessed=2**22,
        ),
        name="attention",
    )(queries, *pieces, *(held or ()))


def out_kernel(back_ref, tok_ref, weight_ref, out_ref):
    half = back_ref.shape[1]
    low, high = [], []
    mask = lanes_of((half, 128)) < HEAD_DIM
    for pair in range(HEADS // 2):
        even = back_ref[2 * pair].astype(F32)
        odd = back_ref[2 * pair + 1].astype(F32)
        low.append(jnp.where(mask, even, pltpu.roll(odd, HEAD_DIM, 1)).astype(BF))
        high.append(jnp.where(mask, pltpu.roll(even, HEAD_DIM, 1), odd).astype(BF))
    attended = jnp.concatenate(
        [jnp.concatenate(low, axis=1), jnp.concatenate(high, axis=1)], axis=0
    )
    mixed = tok_ref[...] + jnp.dot(attended, weight_ref[...], preferred_element_type=F32)
    cols = out_ref.shape[1]
    rows = out_ref.shape[0]
    columns = [mixed[c * rows : (c + 1) * rows] for c in range(cols)]
    out_ref[...] = jnp.stack(columns, axis=1).astype(BF)


def body(surface_field, conv_a, conv_b, norm_gain, qkv_weight, out_weight):
    lon_count = lax.axis_size("lon")
    lat_count = lax.axis_size("lat")
    lat = lax.axis_index("lat")
    rows, cols, chans = surface_field.shape
    forward = [(i, (i + 1) % lon_count) for i in range(lon_count)]
    backward = [(target, source) for source, target in forward]
    swap = [(c, (c + 1) % lat_count) for c in range(lat_count)]
    first_row = jnp.where(lat == 0, rows - REACH, 0)
    edge = lax.ppermute(
        lax.dynamic_slice_in_dim(surface_field, first_row, REACH, axis=0), "lat", swap
    )

    def columns(at):
        beyond = jnp.concatenate([surface_field[:, at : at + REACH], edge[:, at : at + REACH]])
        return beyond.transpose(1, 0, 2)

    low = lax.ppermute(columns(cols - REACH), "lon", forward)
    high = lax.ppermute(columns(0), "lon", backward)
    field = surface_field.transpose(1, 0, 2)
    edge = edge.transpose(1, 0, 2)

    wide_cols = cols + 2 * REACH
    span = -(-(rows + 4) // 16) * 16
    pooled_cols = cols // 2 + 2
    pooled_rows = rows // 2
    count = (rows // 4) * (cols // 4)
    half = count // 2
    slabs = CB // 128
    where = jnp.stack([lat, jnp.int32(lat_count)]).astype(jnp.int32)
    tokens, outgoing = pl.pallas_call(
        conv_kernel,
        out_shape=(
            jax.ShapeDtypeStruct((count, CB), F32),
            jax.ShapeDtypeStruct((HEADS, count + half, 128), BF),
        ),
        in_specs=[SMEM] + [VMEM] * 5 + [HBM] * 3,
        out_specs=(VMEM, VMEM),
        scratch_shapes=[
            pltpu.VMEM((9 * chans, CB), BF),
            pltpu.VMEM((9 * CB, CB), BF),
            pltpu.VMEM(qkv_weight.shape, BF),
            pltpu.VMEM((wide_cols, span + 8, chans), F32),
            pltpu.VMEM((3, wide_cols, span, chans), BF),
            pltpu.VMEM((pooled_cols * slabs, span, 128), F32),
            pltpu.VMEM((3, pooled_cols, pooled_rows, CB), BF),
            pltpu.VMEM((cols // 4 * slabs, pooled_rows, 128), F32),
            pltpu.SemaphoreType.DMA((3,)),
        ],
        compiler_params=pltpu.CompilerParams(vmem_limit_bytes=40 * 2**20),
        name="convs",
    )(
        where, field, low, high, edge, norm_gain.reshape(1, CB),
        *[pltpu.with_memory_space_constraint(w, pltpu.HBM) for w in (conv_a.reshape(9 * chans, CB), conv_b.reshape(9 * CB, CB), qkv_weight)],
    )

    residues = lon_count // HEADS
    groups = [[r * HEADS + h for h in range(HEADS)] for r in range(residues)]
    arrived = lax.all_to_all(outgoing, "lon", 0, 0, axis_index_groups=groups, tiled=True)
    queries = arrived[:, count:].reshape(HEADS * half, 128)
    own = arrived[:, :count].reshape(HEADS * count, 128)

    def beside(value, d):
        pairs = [
            (r * HEADS + h, (r + d) % residues * HEADS + h)
            for r in range(residues)
            for h in range(HEADS)
        ]
        return lax.ppermute(value, "lon", pairs)

    def other(value):
        return lax.ppermute(value, "lat", swap)

    near = beside(own, 1)
    near_back = beside(own, residues - 1)
    far = beside(own, 2)
    own_other = other(own)
    queries, *held = attend(queries, [own, own_other], None, False)
    near_other = other(near)
    near_back_other = other(near_back)
    held = attend(queries, [near, near_back], held, False)
    far_other = other(far)
    held = attend(queries, [near_other, near_back_other], held, False)
    attended = attend(queries, [far, far_other], held, True)
    returned = lax.all_to_all(
        attended.reshape(HEADS, half, 128), "lon", 0, 0, axis_index_groups=groups, tiled=True
    )
    mixed = pl.pallas_call(
        out_kernel,
        out_shape=jax.ShapeDtypeStruct((rows // 4, cols // 4, CB), BF),
        in_specs=[VMEM] * 3,
        out_specs=VMEM,
        compiler_params=pltpu.CompilerParams(vmem_limit_bytes=16 * 2**20),
        name="mix",
    )(returned, tokens, out_weight)
    return mixed


def solution(mesh):
    in_specs = (P(("grp", "lat"), "lon", None), P(), P(), P(), P(), P())
    out_specs = P(("grp", "lat"), "lon", None)
    return jax.shard_map(body, mesh=mesh, in_specs=in_specs, out_specs=out_specs, check_vma=False)
```

```python
import functools
import math

import jax
import jax.numpy as jnp
from jax import lax
from jax.experimental import pallas as pl
from jax.experimental.pallas import tpu as pltpu
from jax.sharding import PartitionSpec as P

CB = 512
HEADS = 16
HEAD_DIM = 64
REACH = 3
BF = jnp.bfloat16
F32 = jnp.float32
VMEM = pl.BlockSpec(memory_space=pltpu.VMEM)
SMEM = pl.BlockSpec(memory_space=pltpu.SMEM)
HBM = pl.BlockSpec(memory_space=pltpu.HBM)


def silu(v):
    half = 0.5 * v
    return half + half * jnp.tanh(half)


def lanes_of(shape):
    return lax.broadcasted_iota(jnp.int32, shape, len(shape) - 1)


def shift_rows(wide, out, rows, ref, edge_rows, lat, last):
    n, span = out.shape[1], out.shape[2]
    wide[:n, REACH : REACH + rows, :] = ref.astype(F32)
    edge_rows = edge_rows.astype(F32)
    nothing = jnp.zeros_like(edge_rows)
    tail = 2 * REACH + rows
    wide[:n, 0:REACH, :] = jnp.where(lat == 0, nothing, edge_rows)
    wide[:n, REACH + rows : tail, :] = jnp.where(lat == last, nothing, edge_rows)
    wide[:n, tail:, :] = jnp.zeros((n, wide.shape[1] - tail, wide.shape[2]), F32)
    for a in range(3):
        out[a] = wide[:n, a : a + span, :].astype(BF)


def first_level(column, weight, span):
    parts = [
        jnp.concatenate([column(a, b), column(a, b + 1)], axis=0)
        for a in range(3)
        for b in range(3)
    ]
    first = silu(jnp.dot(jnp.concatenate(parts, axis=1), weight, preferred_element_type=F32))
    return first[:span] + first[span:]


def store_pair(pool, c, pair, rows, lat, last):
    slabs = CB // 128
    for s in range(slabs):
        pool[c * slabs + s] = pair[:, 128 * s : 128 * (s + 1)]

    @pl.when(lat == 0)
    def _():
        pool[c * slabs : (c + 1) * slabs, 0:2, :] = jnp.zeros((slabs, 2, 128), F32)

    @pl.when(lat == last)
    def _():
        pool[c * slabs : (c + 1) * slabs, rows + 2 : rows + 4, :] = jnp.zeros((slabs, 2, 128), F32)


def middle_kernel(
    lat_ref, mid_ref, edge_ref, conv_a_hbm, shifted, pool, conv_a_ref, wide, sem
):
    copy = pltpu.make_async_copy(conv_a_hbm, conv_a_ref, sem)
    copy.start()
    lat = lat_ref[0]
    last = lat_ref[1] - 1
    cols, rows, _ = mid_ref.shape
    shift_rows(wide, shifted, rows, mid_ref[...], edge_ref[...], lat, last)
    copy.wait()
    for c in range(cols // 2 - 2):
        pair = first_level(
            lambda a, b, c=c: shifted[a, 2 * c + 1 + b], conv_a_ref[...], shifted.shape[2]
        )
        store_pair(pool, c, pair, rows, lat, last)


def conv_kernel(
    lat_ref, shifted, pool_mid, conv_a_ref, low_ref, high_ref, gain_hbm, conv_b_hbm, qkv_hbm,
    tok_ref, out_ref,
    gain_ref, conv_b_ref, qkv_ref, wide, low, high, pool_side, ready, pool_b, sems,
):
    copies = [
        pltpu.make_async_copy(conv_b_hbm, conv_b_ref, sems.at[0]),
        pltpu.make_async_copy(gain_hbm, gain_ref, sems.at[1]),
        pltpu.make_async_copy(qkv_hbm, qkv_ref, sems.at[2]),
    ]
    for copy in copies:
        copy.start()
    lat = lat_ref[0]
    last = lat_ref[1] - 1
    cols, span = shifted.shape[1], shifted.shape[2]
    rows = low_ref.shape[1] - REACH
    slabs = CB // 128
    pooled_cols = cols // 2 + 2
    pooled_rows = rows // 2
    for ref, out in ((low_ref, low), (high_ref, high)):
        shift_rows(wide, out, rows, ref[:, :rows], ref[:, rows:], lat, last)

    def column(a, w):
        if w < REACH:
            return low[a, w]
        if w < REACH + cols:
            return shifted[a, w - REACH]
        return high[a, w - REACH - cols]

    def pooled(c):
        if 2 <= c < pooled_cols - 2:
            return pool_mid, c - 2
        return pool_side, c if c < 2 else c - (pooled_cols - 4)

    for c in range(pooled_cols):
        pool, at = pooled(c)
        if pool is pool_side:
            pair = first_level(
                lambda a, b, c=c: column(a, 2 * c + b), conv_a_ref[...], span
            )
            store_pair(pool, at, pair, rows, lat, last)
        for s in range(slabs):
            for a in range(3):
                even = pool[at * slabs + s, pl.ds(2 * a, pooled_rows, stride=2), :]
                odd = pool[at * slabs + s, pl.ds(2 * a + 1, pooled_rows, stride=2), :]
                ready[a, c, :, 128 * s : 128 * (s + 1)] = ((even + odd) * 0.25).astype(BF)
    copies[0].wait()
    cols_b = cols // 2
    parts = [
        ready[a, b : b + cols_b].reshape(cols_b * pooled_rows, CB)
        for a in range(3)
        for b in range(3)
    ]
    second = silu(
        jnp.dot(jnp.concatenate(parts, axis=1), conv_b_ref[...], preferred_element_type=F32)
    )
    tokens = []
    for c in range(cols_b // 2):
        at = 2 * c * pooled_rows
        pair = second[at : at + pooled_rows] + second[at + pooled_rows : at + 2 * pooled_rows]
        pieces = []
        for s in range(slabs):
            pool_b[c * slabs + s] = pair[:, 128 * s : 128 * (s + 1)]
            even = pool_b[c * slabs + s, pl.ds(0, pooled_rows // 2, stride=2), :]
            odd = pool_b[c * slabs + s, pl.ds(1, pooled_rows // 2, stride=2), :]
            pieces.append((even + odd) * 0.25)
        tokens.append(jnp.concatenate(pieces, axis=1))
    tokens = jnp.concatenate(tokens, axis=0)
    tok_ref[...] = tokens
    centred = tokens - jnp.mean(tokens, axis=-1, keepdims=True)
    spread = jnp.mean(centred * centred, axis=-1, keepdims=True)
    copies[1].wait()
    normed = (centred * lax.rsqrt(spread + 0.01) * gain_ref[...]).astype(BF)
    copies[2].wait()
    width = HEADS * HEAD_DIM
    count = tokens.shape[0]
    half = count // 2
    projected = jnp.dot(normed, qkv_ref[...], preferred_element_type=F32)
    below = lanes_of((count, 128)) < HEAD_DIM
    below_half = lanes_of((half, 128)) < HEAD_DIM
    for pair in range(HEADS // 2):
        q, k, v = (
            projected[:, width * s + 128 * pair : width * s + 128 * (pair + 1)] for s in range(3)
        )
        turned = [pltpu.roll(x, HEAD_DIM, 1) for x in (q, k, v)]
        h = 2 * pair
        out_ref[h, :count] = jnp.where(below, k, turned[2]).astype(BF)
        out_ref[h + 1, :count] = jnp.where(below, turned[1], v).astype(BF)
        out_ref[h, count:] = jnp.where(below_half, q[:half], turned[0][half:]).astype(BF)
        out_ref[h + 1, count:] = jnp.where(below_half, turned[0][:half], q[half:]).astype(BF)


def attention_kernel(first, final, pieces, *refs):
    refs = list(refs)
    q_ref = refs.pop(0)
    kv_refs = [refs.pop(0) for _ in range(pieces)]
    held = None if first else (refs.pop(0), refs.pop(0))
    ones_vals = refs.pop()
    queries, acc_ref, top_ref = (None, None, None) if final else refs if first else (None, *refs)
    keys = kv_refs[0].shape[0]
    mask_keys = lanes_of((keys, 128)) < HEAD_DIM
    if first:
        rows = q_ref.shape[0]
        packed = q_ref[...].astype(F32)
        below = lanes_of((rows, 128)) < HEAD_DIM
        zero = jnp.zeros_like(packed)
        queries[0] = jnp.where(below, packed, zero).astype(BF)
        queries[1] = jnp.where(below, pltpu.roll(packed, HEAD_DIM, 1), zero).astype(BF)
    else:
        queries = q_ref
        rows = q_ref.shape[1]
    one = jnp.ones((keys, 128), BF)
    for i, kv in enumerate(kv_refs):
        ones_vals[i] = jnp.where(mask_keys, one, kv[...])
    factor = HEAD_DIM ** (-0.5) * math.log2(math.e)
    block = rows // 2
    units = [(at, i) for at in range(0, rows, block) for i in range(pieces)]

    def score(unit):
        at, i = unit
        return lax.dot_general(
            queries[:, at : at + block, :].reshape(2 * block, 128),
            kv_refs[i][...],
            (((1,), (1,)), ((), ())),
            preferred_element_type=F32,
        )

    ahead = score(units[0])
    for n, (at, i) in enumerate(units):
        scores = ahead
        if n + 1 < len(units):
            ahead = score(units[n + 1])
        if i == 0:
            if first:
                top = jnp.full((2 * block, 1), -jnp.inf, F32)
                acc = None
            else:
                top = held[1][:, at : at + block, :].reshape(2 * block, 128)[:, :1]
                acc = held[0][:, at : at + block, :].reshape(2 * block, 128)
        new_top = jnp.maximum(top, jnp.max(scores, axis=-1, keepdims=True))
        raised = jnp.exp2((scores - new_top) * factor).astype(BF)
        part = jnp.dot(raised, ones_vals[i], preferred_element_type=F32)
        acc = part if acc is None else acc * jnp.exp2((top - new_top) * factor) + part
        top = new_top
        if i < pieces - 1:
            continue
        if not final:
            acc_ref[:, at : at + block, :] = acc.reshape(2, block, 128)
            wide = jnp.broadcast_to(top, (2 * block, 128))
            top_ref[:, at : at + block, :] = wide.reshape(2, block, 128)
            continue
        turned = pltpu.roll(acc, HEAD_DIM, 1)
        low = turned[:block] / acc[:block]
        high = acc[block:] / turned[block:]
        mask = lanes_of((block, 128)) < HEAD_DIM
        refs[0][at : at + block, :] = jnp.where(mask, low, high).astype(BF)


def attend(queries, pieces, held, final):
    first = held is None
    rows = queries.shape[0] if first else queries.shape[1]
    keys = pieces[0].shape[0]
    state = [jax.ShapeDtypeStruct((2, rows, 128), F32)] * 2
    if final:
        outs = jax.ShapeDtypeStruct((rows, 128), BF)
    else:
        outs = tuple(([jax.ShapeDtypeStruct((2, rows, 128), BF)] if first else []) + state)
    return pl.pallas_call(
        functools.partial(attention_kernel, first, final, len(pieces)),
        out_shape=outs,
        in_specs=[VMEM] * (1 + len(pieces) + (0 if first else 2)),
        out_specs=VMEM if final else (VMEM,) * len(outs),
        scratch_shapes=[pltpu.VMEM((len(pieces), keys, 128), BF)],
        compiler_params=pltpu.CompilerParams(vmem_limit_bytes=24 * 2**20),
        cost_estimate=pl.CostEstimate(
            flops=4 * 2 * rows * len(pieces) * keys * 256,
            transcendentals=2 * rows * len(pieces) * keys,
            bytes_accessed=2**22,
        ),
        name="attention",
    )(queries, *pieces, *(held or ()))


def out_kernel(back_ref, tok_ref, weight_ref, out_ref):
    half = back_ref.shape[1]
    low, high = [], []
    mask = lanes_of((half, 128)) < HEAD_DIM
    for pair in range(HEADS // 2):
        even = back_ref[2 * pair].astype(F32)
        odd = back_ref[2 * pair + 1].astype(F32)
        low.append(jnp.where(mask, even, pltpu.roll(odd, HEAD_DIM, 1)).astype(BF))
        high.append(jnp.where(mask, pltpu.roll(even, HEAD_DIM, 1), odd).astype(BF))
    attended = jnp.concatenate(
        [jnp.concatenate(low, axis=1), jnp.concatenate(high, axis=1)], axis=0
    )
    mixed = tok_ref[...] + jnp.dot(attended, weight_ref[...], preferred_element_type=F32)
    cols = out_ref.shape[1]
    rows = out_ref.shape[0]
    columns = [mixed[c * rows : (c + 1) * rows] for c in range(cols)]
    out_ref[...] = jnp.stack(columns, axis=1).astype(BF)


def body(surface_field, conv_a, conv_b, norm_gain, qkv_weight, out_weight):
    lon_count = lax.axis_size("lon")
    lat_count = lax.axis_size("lat")
    lat = lax.axis_index("lat")
    rows, cols, chans = surface_field.shape
    forward = [(i, (i + 1) % lon_count) for i in range(lon_count)]
    backward = [(target, source) for source, target in forward]
    swap = [(c, (c + 1) % lat_count) for c in range(lat_count)]
    first_row = jnp.where(lat == 0, rows - REACH, 0)
    edge = lax.ppermute(
        lax.dynamic_slice_in_dim(surface_field, first_row, REACH, axis=0), "lat", swap
    )

    def columns(at):
        beyond = jnp.concatenate([surface_field[:, at : at + REACH], edge[:, at : at + REACH]])
        return beyond.transpose(1, 0, 2)

    low = lax.ppermute(columns(cols - REACH), "lon", forward)
    high = lax.ppermute(columns(0), "lon", backward)
    field = surface_field.transpose(1, 0, 2)
    edge = edge.transpose(1, 0, 2)

    span = -(-(rows + 4) // 16) * 16
    pooled_cols = cols // 2 + 2
    pooled_rows = rows // 2
    count = (rows // 4) * (cols // 4)
    half = count // 2
    slabs = CB // 128
    where = jnp.stack([lat, jnp.int32(lat_count)]).astype(jnp.int32)

    def in_hbm(value):
        return pltpu.with_memory_space_constraint(value, pltpu.HBM)

    shifted, pool_mid, conv_a_here = pl.pallas_call(
        middle_kernel,
        out_shape=(
            jax.ShapeDtypeStruct((3, cols, span, chans), BF),
            jax.ShapeDtypeStruct(((pooled_cols - 4) * slabs, span, 128), F32),
            jax.ShapeDtypeStruct((9 * chans, CB), BF),
        ),
        in_specs=[SMEM, VMEM, VMEM, HBM],
        out_specs=(VMEM,) * 3,
        scratch_shapes=[
            pltpu.VMEM((cols, span + 8, chans), F32),
            pltpu.SemaphoreType.DMA,
        ],
        compiler_params=pltpu.CompilerParams(vmem_limit_bytes=16 * 2**20),
        name="middle",
    )(where, field, edge, in_hbm(conv_a.reshape(9 * chans, CB)))
    tokens, outgoing = pl.pallas_call(
        conv_kernel,
        out_shape=(
            jax.ShapeDtypeStruct((count, CB), F32),
            jax.ShapeDtypeStruct((HEADS, count + half, 128), BF),
        ),
        in_specs=[SMEM] + [VMEM] * 5 + [HBM] * 3,
        out_specs=(VMEM, VMEM),
        scratch_shapes=[
            pltpu.VMEM((1, CB), F32),
            pltpu.VMEM((9 * CB, CB), BF),
            pltpu.VMEM(qkv_weight.shape, BF),
            pltpu.VMEM((REACH, span + 8, chans), F32),
            pltpu.VMEM((3, REACH, span, chans), BF),
            pltpu.VMEM((3, REACH, span, chans), BF),
            pltpu.VMEM((4 * slabs, span, 128), F32),
            pltpu.VMEM((3, pooled_cols, pooled_rows, CB), BF),
            pltpu.VMEM((cols // 4 * slabs, pooled_rows, 128), F32),
            pltpu.SemaphoreType.DMA((3,)),
        ],
        compiler_params=pltpu.CompilerParams(vmem_limit_bytes=32 * 2**20),
        name="convs",
    )(
        where, shifted, pool_mid, conv_a_here, low, high,
        in_hbm(norm_gain.reshape(1, CB)), in_hbm(conv_b.reshape(9 * CB, CB)), in_hbm(qkv_weight),
    )

    residues = lon_count // HEADS
    groups = [[r * HEADS + h for h in range(HEADS)] for r in range(residues)]
    arrived = lax.all_to_all(outgoing, "lon", 0, 0, axis_index_groups=groups, tiled=True)
    queries = arrived[:, count:].reshape(HEADS * half, 128)
    own = arrived[:, :count].reshape(HEADS * count, 128)

    def beside(value, d):
        pairs = [
            (r * HEADS + h, (r + d) % residues * HEADS + h)
            for r in range(residues)
            for h in range(HEADS)
        ]
        return lax.ppermute(value, "lon", pairs)

    def other(value):
        return lax.ppermute(value, "lat", swap)

    near = beside(own, 1)
    near_back = beside(own, residues - 1)
    queries, *held = attend(queries, [own], None, False)
    own_other = other(own)
    far = beside(own, 2)
    held = attend(queries, [own_other], held, False)
    near_other = other(near)
    near_back_other = other(near_back)
    held = attend(queries, [near, near_back], held, False)
    far_other = other(far)
    held = attend(queries, [near_other, near_back_other], held, False)
    attended = attend(queries, [far, far_other], held, True)
    returned = lax.all_to_all(
        attended.reshape(HEADS, half, 128), "lon", 0, 0, axis_index_groups=groups, tiled=True
    )
    mixed = pl.pallas_call(
        out_kernel,
        out_shape=jax.ShapeDtypeStruct((rows // 4, cols // 4, CB), BF),
        in_specs=[VMEM] * 3,
        out_specs=VMEM,
        compiler_params=pltpu.CompilerParams(vmem_limit_bytes=16 * 2**20),
        name="mix",
    )(returned, tokens, out_weight)
    return mixed


def solution(mesh):
    in_specs = (P(("grp", "lat"), "lon", None), P(), P(), P(), P(), P())
    out_specs = P(("grp", "lat"), "lon", None)
    return jax.shard_map(body, mesh=mesh, in_specs=in_specs, out_specs=out_specs, check_vma=False)
```

```python
import functools
import math

import jax
import jax.numpy as jnp
from jax import lax
from jax.experimental import pallas as pl
from jax.experimental.pallas import tpu as pltpu
from jax.sharding import PartitionSpec as P

CB = 512
HEADS = 16
HEAD_DIM = 64
REACH = 3
BF = jnp.bfloat16
F32 = jnp.float32
VMEM = pl.BlockSpec(memory_space=pltpu.VMEM)
SMEM = pl.BlockSpec(memory_space=pltpu.SMEM)
HBM = pl.BlockSpec(memory_space=pltpu.HBM)


def silu(v):
    half = 0.5 * v
    return half + half * jnp.tanh(half)


def lanes_of(shape):
    return lax.broadcasted_iota(jnp.int32, shape, len(shape) - 1)


def shift_rows(wide, out, rows, ref, edge_rows, lat, last):
    n, span = out.shape[1], out.shape[2]
    wide[:n, REACH : REACH + rows, :] = ref
    nothing = jnp.zeros_like(edge_rows)
    tail = 2 * REACH + rows
    wide[:n, 0:REACH, :] = jnp.where(lat == 0, nothing, edge_rows)
    wide[:n, REACH + rows : tail, :] = jnp.where(lat == last, nothing, edge_rows)
    wide[:n, tail:, :] = jnp.zeros((n, wide.shape[1] - tail, wide.shape[2]), F32)
    for a in range(3):
        out[a] = wide[:n, a : a + span, :].astype(BF)


def first_level(column, firsts, weight, span):
    parts = [
        jnp.concatenate([column(a, w + b + n) for w in firsts for n in (0, 1)], axis=0)
        for a in range(3)
        for b in range(3)
    ]
    first = silu(jnp.dot(jnp.concatenate(parts, axis=1), weight, preferred_element_type=F32))
    return [
        first[2 * n * span : (2 * n + 1) * span] + first[(2 * n + 1) * span : (2 * n + 2) * span]
        for n in range(len(firsts))
    ]


def store_pair(pool, c, pair, rows, lat, last):
    slabs = CB // 128
    for s in range(slabs):
        pool[c * slabs + s] = pair[:, 128 * s : 128 * (s + 1)]

    @pl.when(lat == 0)
    def _():
        pool[c * slabs : (c + 1) * slabs, 0:2, :] = jnp.zeros((slabs, 2, 128), F32)

    @pl.when(lat == last)
    def _():
        pool[c * slabs : (c + 1) * slabs, rows + 2 : rows + 4, :] = jnp.zeros((slabs, 2, 128), F32)


def pool_rows(pool, at, ready, c):
    slabs = CB // 128
    count = ready.shape[2]
    for s in range(slabs):
        for a in range(3):
            even = pool[at * slabs + s, pl.ds(2 * a, count, stride=2), :]
            odd = pool[at * slabs + s, pl.ds(2 * a + 1, count, stride=2), :]
            ready[a, c, :, 128 * s : 128 * (s + 1)] = ((even + odd) * 0.25).astype(BF)


def middle_kernel(
    lat_ref, mid_ref, edge_ref, conv_a_hbm, conv_b_hbm, qkv_hbm,
    shifted, ready, conv_a_ref, conv_b_ref, qkv_ref,
    wide, pool, sems,
):
    copies = [
        pltpu.make_async_copy(conv_a_hbm, conv_a_ref, sems.at[0]),
        pltpu.make_async_copy(conv_b_hbm, conv_b_ref, sems.at[1]),
        pltpu.make_async_copy(qkv_hbm, qkv_ref, sems.at[2]),
    ]
    for copy in copies:
        copy.start()
    lat = lat_ref[0]
    last = lat_ref[1] - 1
    cols, rows, _ = mid_ref.shape
    shift_rows(
        wide, shifted, rows, mid_ref[...].astype(F32), edge_ref[...].astype(F32), lat, last
    )
    copies[0].wait()
    firsts = [2 * c + 1 for c in range(cols // 2 - 2)]
    pairs = first_level(lambda a, w: shifted[a, w], firsts, conv_a_ref[...], shifted.shape[2])
    for c, pair in enumerate(pairs):
        store_pair(pool, c, pair, rows, lat, last)
        pool_rows(pool, c, ready, c)
    copies[1].wait()
    copies[2].wait()


def conv_kernel(
    lat_ref, shifted, ready_mid, conv_a_ref, conv_b_ref, qkv_ref, pair_ref, next_ref, gain_ref,
    tok_ref, out_ref,
    wide, low, high, pool_side, ready, pool_b,
):
    lat = lat_ref[0]
    last = lat_ref[1] - 1
    cols, span = shifted.shape[1], shifted.shape[2]
    rows = pair_ref.shape[1] - REACH
    even = lat_ref[2] == 0
    slabs = CB // 128
    pooled_cols = cols // 2 + 2
    pooled_rows = rows // 2
    of_pair = pair_ref[...].astype(F32)
    of_next = next_ref[...].astype(F32)
    for out, value in (
        (low, jnp.where(even, of_next, of_pair)),
        (high, jnp.where(even, of_pair, of_next)),
    ):
        shift_rows(wide, out, rows, value[:, :rows], value[:, rows:], lat, last)

    def column(a, w):
        if w < REACH:
            return low[a, w]
        if w < REACH + cols:
            return shifted[a, w - REACH]
        return high[a, w - REACH - cols]

    for at, group in ((0, (0, 1)), (2, (pooled_cols - 2, pooled_cols - 1))):
        pairs = first_level(column, [2 * c for c in group], conv_a_ref[...], span)
        for n, pair in enumerate(pairs):
            store_pair(pool_side, at + n, pair, rows, lat, last)
            pool_rows(pool_side, at + n, ready, at + n)

    def pooled(a, c):
        if 2 <= c < pooled_cols - 2:
            return ready_mid[a, c - 2]
        return ready[a, c if c < 2 else c - (pooled_cols - 4)]

    cols_b = cols // 2
    parts = [
        jnp.concatenate([pooled(a, c + b) for c in range(cols_b)], axis=0)
        for a in range(3)
        for b in range(3)
    ]
    second = silu(
        jnp.dot(jnp.concatenate(parts, axis=1), conv_b_ref[...], preferred_element_type=F32)
    )
    tokens = []
    for c in range(cols_b // 2):
        at = 2 * c * pooled_rows
        pair = second[at : at + pooled_rows] + second[at + pooled_rows : at + 2 * pooled_rows]
        pieces = []
        for s in range(slabs):
            pool_b[c * slabs + s] = pair[:, 128 * s : 128 * (s + 1)]
            even = pool_b[c * slabs + s, pl.ds(0, pooled_rows // 2, stride=2), :]
            odd = pool_b[c * slabs + s, pl.ds(1, pooled_rows // 2, stride=2), :]
            pieces.append((even + odd) * 0.25)
        tokens.append(jnp.concatenate(pieces, axis=1))
    tokens = jnp.concatenate(tokens, axis=0)
    tok_ref[...] = tokens
    centred = tokens - jnp.mean(tokens, axis=-1, keepdims=True)
    spread = jnp.mean(centred * centred, axis=-1, keepdims=True)
    normed = (centred * lax.rsqrt(spread + 0.01) * gain_ref[...]).astype(BF)
    width = HEADS * HEAD_DIM
    count = tokens.shape[0]
    half = count // 2
    projected = jnp.dot(normed, qkv_ref[...], preferred_element_type=F32)
    below = lanes_of((count, 128)) < HEAD_DIM
    below_half = lanes_of((half, 128)) < HEAD_DIM
    for pair in range(HEADS // 2):
        q, k, v = (
            projected[:, width * s + 128 * pair : width * s + 128 * (pair + 1)] for s in range(3)
        )
        turned = [pltpu.roll(x, HEAD_DIM, 1) for x in (q, k, v)]
        h = 2 * pair
        out_ref[h, :count] = jnp.where(below, k, turned[2]).astype(BF)
        out_ref[h + 1, :count] = jnp.where(below, turned[1], v).astype(BF)
        out_ref[h, count:] = jnp.where(below_half, q[:half], turned[0][half:]).astype(BF)
        out_ref[h + 1, count:] = jnp.where(below_half, turned[0][:half], q[half:]).astype(BF)


def attention_kernel(first, final, pieces, *refs):
    refs = list(refs)
    q_ref = refs.pop(0)
    kv_refs = [[refs.pop(0) for _ in range(n)] for n in pieces]
    pieces = len(kv_refs)
    held = None if first else (refs.pop(0), refs.pop(0))
    ones_vals = refs.pop()
    queries, acc_ref, top_ref = (None, None, None) if final else refs if first else (None, *refs)
    keys = ones_vals.shape[1]

    def piece(i):
        parts = [ref[...] for ref in kv_refs[i]]
        return parts[0] if len(parts) == 1 else jnp.concatenate(parts, axis=0)

    mask_keys = lanes_of((keys, 128)) < HEAD_DIM
    if first:
        rows = q_ref.shape[0]
        packed = q_ref[...].astype(F32)
        below = lanes_of((rows, 128)) < HEAD_DIM
        zero = jnp.zeros_like(packed)
        queries[0] = jnp.where(below, packed, zero).astype(BF)
        queries[1] = jnp.where(below, pltpu.roll(packed, HEAD_DIM, 1), zero).astype(BF)
    else:
        queries = q_ref
        rows = q_ref.shape[1]
    one = jnp.ones((keys, 128), BF)
    for i in range(pieces):
        ones_vals[i] = jnp.where(mask_keys, one, piece(i))
    factor = HEAD_DIM ** (-0.5) * math.log2(math.e)
    block = rows // 2
    units = [(at, i) for at in range(0, rows, block) for i in range(pieces)]

    def score(unit):
        at, i = unit
        return lax.dot_general(
            queries[:, at : at + block, :].reshape(2 * block, 128),
            piece(i),
            (((1,), (1,)), ((), ())),
            preferred_element_type=F32,
        )

    ahead = score(units[0])
    for n, (at, i) in enumerate(units):
        scores = ahead
        if n + 1 < len(units):
            ahead = score(units[n + 1])
        if i == 0:
            if first:
                top = jnp.full((2 * block, 1), -jnp.inf, F32)
                acc = None
            else:
                top = held[1][:, at : at + block, :].reshape(2 * block, 128)[:, :1]
                acc = held[0][:, at : at + block, :].reshape(2 * block, 128)
        new_top = jnp.maximum(top, jnp.max(scores, axis=-1, keepdims=True))
        raised = jnp.exp2((scores - new_top) * factor).astype(BF)
        part = jnp.dot(raised, ones_vals[i], preferred_element_type=F32)
        acc = part if acc is None else acc * jnp.exp2((top - new_top) * factor) + part
        top = new_top
        if i < pieces - 1:
            continue
        if not final:
            acc_ref[:, at : at + block, :] = acc.reshape(2, block, 128)
            wide = jnp.broadcast_to(top, (2 * block, 128))
            top_ref[:, at : at + block, :] = wide.reshape(2, block, 128)
            continue
        turned = pltpu.roll(acc, HEAD_DIM, 1)
        low = turned[:block] / acc[:block]
        high = acc[block:] / turned[block:]
        mask = lanes_of((block, 128)) < HEAD_DIM
        refs[0][at : at + block, :] = jnp.where(mask, low, high).astype(BF)


def attend(queries, pieces, held, final):
    first = held is None
    rows = queries.shape[0] if first else queries.shape[1]
    keys = sum(part.shape[0] for part in pieces[0])
    parts = [part for piece in pieces for part in piece]
    state = [jax.ShapeDtypeStruct((2, rows, 128), F32)] * 2
    if final:
        outs = jax.ShapeDtypeStruct((rows, 128), BF)
    else:
        outs = tuple(([jax.ShapeDtypeStruct((2, rows, 128), BF)] if first else []) + state)
    return pl.pallas_call(
        functools.partial(attention_kernel, first, final, [len(piece) for piece in pieces]),
        out_shape=outs,
        in_specs=[VMEM] * (1 + len(parts) + (0 if first else 2)),
        out_specs=VMEM if final else (VMEM,) * len(outs),
        scratch_shapes=[pltpu.VMEM((len(pieces), keys, 128), BF)],
        compiler_params=pltpu.CompilerParams(vmem_limit_bytes=24 * 2**20),
        cost_estimate=pl.CostEstimate(
            flops=4 * 2 * rows * len(pieces) * keys * 256,
            transcendentals=2 * rows * len(pieces) * keys,
            bytes_accessed=2**22,
        ),
        name="attention",
    )(queries, *parts, *(held or ()))


def out_kernel(back_ref, tok_ref, weight_ref, out_ref):
    half = back_ref.shape[1]
    low, high = [], []
    mask = lanes_of((half, 128)) < HEAD_DIM
    for pair in range(HEADS // 2):
        even = back_ref[2 * pair].astype(F32)
        odd = back_ref[2 * pair + 1].astype(F32)
        low.append(jnp.where(mask, even, pltpu.roll(odd, HEAD_DIM, 1)).astype(BF))
        high.append(jnp.where(mask, pltpu.roll(even, HEAD_DIM, 1), odd).astype(BF))
    attended = jnp.concatenate(
        [jnp.concatenate(low, axis=1), jnp.concatenate(high, axis=1)], axis=0
    )
    mixed = tok_ref[...] + jnp.dot(attended, weight_ref[...], preferred_element_type=F32)
    cols = out_ref.shape[1]
    rows = out_ref.shape[0]
    columns = [mixed[c * rows : (c + 1) * rows] for c in range(cols)]
    out_ref[...] = jnp.stack(columns, axis=1).astype(BF)


def swaps(offset, count, stride):
    pairs = []
    for i in range(0, count, 2):
        one, two = offset(i) % count, (offset(i) + 1) % count
        for s in range(stride):
            pairs += [(one * stride + s, two * stride + s), (two * stride + s, one * stride + s)]
    return pairs


def body(surface_field, conv_a, conv_b, norm_gain, qkv_weight, out_weight):
    lon_count = lax.axis_size("lon")
    lat_count = lax.axis_size("lat")
    lat = lax.axis_index("lat")
    rows, cols, chans = surface_field.shape
    lon = lax.axis_index("lon")
    even = lon % 2 == 0
    swap = [(c, (c + 1) % lat_count) for c in range(lat_count)]
    first_row = jnp.where(lat == 0, rows - REACH, 0)
    edge = lax.ppermute(
        lax.dynamic_slice_in_dim(surface_field, first_row, REACH, axis=0), "lat", swap
    )

    def columns(at):
        beyond = jnp.concatenate([surface_field[:, at : at + REACH], edge[:, at : at + REACH]])
        return beyond.transpose(1, 0, 2)

    above, below = columns(cols - REACH), columns(0)
    of_pair = lax.ppermute(jnp.where(even, above, below), "lon", swaps(lambda i: i, lon_count, 1))
    of_next = lax.ppermute(
        jnp.where(even, below, above), "lon", swaps(lambda i: i + 1, lon_count, 1)
    )
    field = surface_field.transpose(1, 0, 2)
    edge = edge.transpose(1, 0, 2)

    span = -(-(rows + 4) // 16) * 16
    pooled_cols = cols // 2 + 2
    pooled_rows = rows // 2
    count = (rows // 4) * (cols // 4)
    half = count // 2
    slabs = CB // 128
    where = jnp.stack([lat, jnp.int32(lat_count), lon % 2]).astype(jnp.int32)

    def in_hbm(value):
        return pltpu.with_memory_space_constraint(value, pltpu.HBM)

    weights = (conv_a.reshape(9 * chans, CB), conv_b.reshape(9 * CB, CB), qkv_weight)
    shifted, ready_mid, *here = pl.pallas_call(
        middle_kernel,
        out_shape=(
            jax.ShapeDtypeStruct((3, cols, span, chans), BF),
            jax.ShapeDtypeStruct((3, pooled_cols - 4, pooled_rows, CB), BF),
        )
        + tuple(jax.ShapeDtypeStruct(w.shape, BF) for w in weights),
        in_specs=[SMEM, VMEM, VMEM] + [HBM] * 3,
        out_specs=(VMEM,) * 5,
        scratch_shapes=[
            pltpu.VMEM((cols, span + 8, chans), F32),
            pltpu.VMEM(((pooled_cols - 4) * slabs, span, 128), F32),
            pltpu.SemaphoreType.DMA((3,)),
        ],
        compiler_params=pltpu.CompilerParams(vmem_limit_bytes=24 * 2**20),
        name="middle",
    )(where, field, edge, *[in_hbm(w) for w in weights])
    tokens, outgoing = pl.pallas_call(
        conv_kernel,
        out_shape=(
            jax.ShapeDtypeStruct((count, CB), F32),
            jax.ShapeDtypeStruct((HEADS, count + half, 128), BF),
        ),
        in_specs=[SMEM] + [VMEM] * 8,
        out_specs=(VMEM, VMEM),
        scratch_shapes=[
            pltpu.VMEM((REACH, span + 8, chans), F32),
            pltpu.VMEM((3, REACH, span, chans), BF),
            pltpu.VMEM((3, REACH, span, chans), BF),
            pltpu.VMEM((4 * slabs, span, 128), F32),
            pltpu.VMEM((3, 4, pooled_rows, CB), BF),
            pltpu.VMEM((cols // 4 * slabs, pooled_rows, 128), F32),
        ],
        compiler_params=pltpu.CompilerParams(vmem_limit_bytes=24 * 2**20),
        name="convs",
    )(where, shifted, ready_mid, *here, of_pair, of_next, norm_gain.reshape(1, CB))

    residues = lon_count // HEADS
    groups = [[r * HEADS + h for h in range(HEADS)] for r in range(residues)]
    arrived = lax.all_to_all(outgoing, "lon", 0, 0, axis_index_groups=groups, tiled=True)
    queries = arrived[:, count:].reshape(HEADS * half, 128)
    own = arrived[:, :count].reshape(HEADS * count, 128)

    def other(value):
        return lax.ppermute(value, "lat", swap)

    def pair_swap(value):
        return lax.ppermute(value, "lon", swaps(lambda i: i, residues, HEADS))

    def next_swap(value):
        return lax.ppermute(value, "lon", swaps(lambda i: i + 1, residues, HEADS))

    near = pair_swap(own)
    near_back = next_swap(own)
    queries, *held = attend(queries, [(own,)], None, False)
    own_other = other(own)
    held = attend(queries, [(own_other,)], held, False)
    middle = own.shape[0] // 2
    far_a = pair_swap(near_back[:middle])
    far_b = next_swap(near[middle:])
    near_other = other(near)
    near_back_other = other(near_back)
    held = attend(queries, [(near,), (near_back,)], held, False)
    held = attend(queries, [(near_other,), (near_back_other,)], held, False)
    far_a_other = other(far_a)
    far_b_other = other(far_b)
    held = attend(queries, [(far_a, far_b)], held, False)
    attended = attend(queries, [(far_a_other, far_b_other)], held, True)
    returned = lax.all_to_all(
        attended.reshape(HEADS, half, 128), "lon", 0, 0, axis_index_groups=groups, tiled=True
    )
    mixed = pl.pallas_call(
        out_kernel,
        out_shape=jax.ShapeDtypeStruct((rows // 4, cols // 4, CB), BF),
        in_specs=[VMEM] * 3,
        out_specs=VMEM,
        compiler_params=pltpu.CompilerParams(vmem_limit_bytes=16 * 2**20),
        name="mix",
    )(returned, tokens, out_weight)
    return mixed


def solution(mesh):
    in_specs = (P(("grp", "lat"), "lon", None), P(), P(), P(), P(), P())
    out_specs = P(("grp", "lat"), "lon", None)
    return jax.shard_map(body, mesh=mesh, in_specs=in_specs, out_specs=out_specs, check_vma=False)
```

```python
import functools
import math

import jax
import jax.numpy as jnp
from jax import lax
from jax.experimental import pallas as pl
from jax.experimental.pallas import tpu as pltpu
from jax.sharding import PartitionSpec as P

CB = 512
HEADS = 16
HEAD_DIM = 64
REACH = 3
BF = jnp.bfloat16
F32 = jnp.float32
VMEM = pl.BlockSpec(memory_space=pltpu.VMEM)
SMEM = pl.BlockSpec(memory_space=pltpu.SMEM)
HBM = pl.BlockSpec(memory_space=pltpu.HBM)


def silu(v):
    half = 0.5 * v
    return half + half * jnp.tanh(half)


def lanes_of(shape):
    return lax.broadcasted_iota(jnp.int32, shape, len(shape) - 1)


def shift_rows(wide, out, rows, ref, edge_rows, lat, last):
    n, span = out.shape[1], out.shape[2]
    wide[:n, REACH : REACH + rows, :] = ref
    nothing = jnp.zeros_like(edge_rows)
    tail = 2 * REACH + rows
    wide[:n, 0:REACH, :] = jnp.where(lat == 0, nothing, edge_rows)
    wide[:n, REACH + rows : tail, :] = jnp.where(lat == last, nothing, edge_rows)
    wide[:n, tail:, :] = jnp.zeros((n, wide.shape[1] - tail, wide.shape[2]), F32)
    for a in range(3):
        out[a] = wide[:n, a : a + span, :].astype(BF)


def first_level(column, firsts, weight, span):
    parts = [
        jnp.concatenate([column(a, w + b + n) for w in firsts for n in (0, 1)], axis=0)
        for a in range(3)
        for b in range(3)
    ]
    first = silu(jnp.dot(jnp.concatenate(parts, axis=1), weight, preferred_element_type=F32))
    return [
        first[2 * n * span : (2 * n + 1) * span] + first[(2 * n + 1) * span : (2 * n + 2) * span]
        for n in range(len(firsts))
    ]


def store_pair(pool, c, pair, rows, lat, last):
    slabs = CB // 128
    for s in range(slabs):
        pool[c * slabs + s] = pair[:, 128 * s : 128 * (s + 1)]

    @pl.when(lat == 0)
    def _():
        pool[c * slabs : (c + 1) * slabs, 0:2, :] = jnp.zeros((slabs, 2, 128), F32)

    @pl.when(lat == last)
    def _():
        pool[c * slabs : (c + 1) * slabs, rows + 2 : rows + 4, :] = jnp.zeros((slabs, 2, 128), F32)


def pool_rows(pool, at, ready, c):
    slabs = CB // 128
    count = ready.shape[2]
    for s in range(slabs):
        for a in range(3):
            even = pool[at * slabs + s, pl.ds(2 * a, count, stride=2), :]
            odd = pool[at * slabs + s, pl.ds(2 * a + 1, count, stride=2), :]
            ready[a, c, :, 128 * s : 128 * (s + 1)] = ((even + odd) * 0.25).astype(BF)


def middle_kernel(
    lat_ref, mid_ref, edge_ref, conv_a_hbm, conv_b_hbm, qkv_hbm,
    shifted, ready, conv_a_ref, conv_b_ref, qkv_ref,
    wide, pool, sems,
):
    copies = [
        pltpu.make_async_copy(conv_a_hbm, conv_a_ref, sems.at[0]),
        pltpu.make_async_copy(conv_b_hbm, conv_b_ref, sems.at[1]),
        pltpu.make_async_copy(qkv_hbm, qkv_ref, sems.at[2]),
    ]
    for copy in copies:
        copy.start()
    lat = lat_ref[0]
    last = lat_ref[1] - 1
    cols, rows, _ = mid_ref.shape
    shift_rows(
        wide, shifted, rows, mid_ref[...].astype(F32), edge_ref[...].astype(F32), lat, last
    )
    copies[0].wait()
    firsts = [2 * c + 1 for c in range(cols // 2 - 2)]
    pairs = first_level(lambda a, w: shifted[a, w], firsts, conv_a_ref[...], shifted.shape[2])
    for c, pair in enumerate(pairs):
        store_pair(pool, c, pair, rows, lat, last)
        pool_rows(pool, c, ready, c)
    copies[1].wait()
    copies[2].wait()


def conv_kernel(
    lat_ref, shifted, ready_mid, conv_a_ref, conv_b_ref, qkv_ref, pair_ref, next_ref, gain_ref,
    tok_ref, out_ref,
    wide, low, high, pool_side, ready, pool_b,
):
    lat = lat_ref[0]
    last = lat_ref[1] - 1
    cols, span = shifted.shape[1], shifted.shape[2]
    rows = pair_ref.shape[1] - REACH
    even = lat_ref[2] == 0
    slabs = CB // 128
    pooled_cols = cols // 2 + 2
    pooled_rows = rows // 2
    of_pair = pair_ref[...].astype(F32)
    of_next = next_ref[...].astype(F32)
    for out, value in (
        (low, jnp.where(even, of_next, of_pair)),
        (high, jnp.where(even, of_pair, of_next)),
    ):
        shift_rows(wide, out, rows, value[:, :rows], value[:, rows:], lat, last)

    def column(a, w):
        if w < REACH:
            return low[a, w]
        if w < REACH + cols:
            return shifted[a, w - REACH]
        return high[a, w - REACH - cols]

    for at, group in ((0, (0, 1, pooled_cols - 2, pooled_cols - 1)),):
        pairs = first_level(column, [2 * c for c in group], conv_a_ref[...], span)
        for n, pair in enumerate(pairs):
            store_pair(pool_side, at + n, pair, rows, lat, last)
            pool_rows(pool_side, at + n, ready, at + n)

    def pooled(a, c):
        if 2 <= c < pooled_cols - 2:
            return ready_mid[a, c - 2]
        return ready[a, c if c < 2 else c - (pooled_cols - 4)]

    cols_b = cols // 2
    parts = [
        jnp.concatenate([pooled(a, c + b) for c in range(cols_b)], axis=0)
        for a in range(3)
        for b in range(3)
    ]
    second = silu(
        jnp.dot(jnp.concatenate(parts, axis=1), conv_b_ref[...], preferred_element_type=F32)
    )
    tokens = []
    for c in range(cols_b // 2):
        at = 2 * c * pooled_rows
        pair = second[at : at + pooled_rows] + second[at + pooled_rows : at + 2 * pooled_rows]
        pieces = []
        for s in range(slabs):
            pool_b[c * slabs + s] = pair[:, 128 * s : 128 * (s + 1)]
            even = pool_b[c * slabs + s, pl.ds(0, pooled_rows // 2, stride=2), :]
            odd = pool_b[c * slabs + s, pl.ds(1, pooled_rows // 2, stride=2), :]
            pieces.append((even + odd) * 0.25)
        tokens.append(jnp.concatenate(pieces, axis=1))
    tokens = jnp.concatenate(tokens, axis=0)
    tok_ref[...] = tokens
    centred = tokens - jnp.mean(tokens, axis=-1, keepdims=True)
    spread = jnp.mean(centred * centred, axis=-1, keepdims=True)
    normed = (centred * lax.rsqrt(spread + 0.01) * gain_ref[...]).astype(BF)
    width = HEADS * HEAD_DIM
    count = tokens.shape[0]
    half = count // 2
    projected = jnp.dot(normed, qkv_ref[...], preferred_element_type=F32)
    below = lanes_of((count, 128)) < HEAD_DIM
    below_half = lanes_of((half, 128)) < HEAD_DIM
    for pair in range(HEADS // 2):
        q, k, v = (
            projected[:, width * s + 128 * pair : width * s + 128 * (pair + 1)] for s in range(3)
        )
        turned = [pltpu.roll(x, HEAD_DIM, 1) for x in (q, k, v)]
        h = 2 * pair
        out_ref[h, :count] = jnp.where(below, k, turned[2]).astype(BF)
        out_ref[h + 1, :count] = jnp.where(below, turned[1], v).astype(BF)
        out_ref[h, count:] = jnp.where(below_half, q[:half], turned[0][half:]).astype(BF)
        out_ref[h + 1, count:] = jnp.where(below_half, turned[0][:half], q[half:]).astype(BF)


def attention_kernel(first, final, pieces, *refs):
    refs = list(refs)
    q_ref = refs.pop(0)
    kv_refs = [[refs.pop(0) for _ in range(n)] for n in pieces]
    pieces = len(kv_refs)
    held = None if first else (refs.pop(0), refs.pop(0))
    ones_vals = refs.pop()
    queries, acc_ref, top_ref = (None, None, None) if final else refs if first else (None, *refs)
    keys = ones_vals.shape[1]

    def piece(i):
        parts = [ref[...] for ref in kv_refs[i]]
        return parts[0] if len(parts) == 1 else jnp.concatenate(parts, axis=0)

    mask_keys = lanes_of((keys, 128)) < HEAD_DIM
    if first:
        rows = q_ref.shape[0]
        packed = q_ref[...].astype(F32)
        below = lanes_of((rows, 128)) < HEAD_DIM
        zero = jnp.zeros_like(packed)
        queries[0] = jnp.where(below, packed, zero).astype(BF)
        queries[1] = jnp.where(below, pltpu.roll(packed, HEAD_DIM, 1), zero).astype(BF)
    else:
        queries = q_ref
        rows = q_ref.shape[1]
    one = jnp.ones((keys, 128), BF)
    for i in range(pieces):
        ones_vals[i] = jnp.where(mask_keys, one, piece(i))
    factor = HEAD_DIM ** (-0.5) * math.log2(math.e)
    block = rows // 2
    units = [(at, i) for at in range(0, rows, block) for i in range(pieces)]

    def score(unit):
        at, i = unit
        return lax.dot_general(
            queries[:, at : at + block, :].reshape(2 * block, 128),
            piece(i),
            (((1,), (1,)), ((), ())),
            preferred_element_type=F32,
        )

    ahead = score(units[0])
    for n, (at, i) in enumerate(units):
        scores = ahead
        if n + 1 < len(units):
            ahead = score(units[n + 1])
        if i == 0:
            if first:
                top = jnp.full((2 * block, 1), -jnp.inf, F32)
                acc = None
            else:
                top = held[1][:, at : at + block, :].reshape(2 * block, 128)[:, :1]
                acc = held[0][:, at : at + block, :].reshape(2 * block, 128)
        new_top = jnp.maximum(top, jnp.max(scores, axis=-1, keepdims=True))
        raised = jnp.exp2((scores - new_top) * factor).astype(BF)
        part = jnp.dot(raised, ones_vals[i], preferred_element_type=F32)
        acc = part if acc is None else acc * jnp.exp2((top - new_top) * factor) + part
        top = new_top
        if i < pieces - 1:
            continue
        if not final:
            acc_ref[:, at : at + block, :] = acc.reshape(2, block, 128)
            wide = jnp.broadcast_to(top, (2 * block, 128))
            top_ref[:, at : at + block, :] = wide.reshape(2, block, 128)
            continue
        turned = pltpu.roll(acc, HEAD_DIM, 1)
        low = turned[:block] / acc[:block]
        high = acc[block:] / turned[block:]
        mask = lanes_of((block, 128)) < HEAD_DIM
        refs[0][at : at + block, :] = jnp.where(mask, low, high).astype(BF)


def attend(queries, pieces, held, final):
    first = held is None
    rows = queries.shape[0] if first else queries.shape[1]
    keys = sum(part.shape[0] for part in pieces[0])
    parts = [part for piece in pieces for part in piece]
    state = [jax.ShapeDtypeStruct((2, rows, 128), F32)] * 2
    if final:
        outs = jax.ShapeDtypeStruct((rows, 128), BF)
    else:
        outs = tuple(([jax.ShapeDtypeStruct((2, rows, 128), BF)] if first else []) + state)
    return pl.pallas_call(
        functools.partial(attention_kernel, first, final, [len(piece) for piece in pieces]),
        out_shape=outs,
        in_specs=[VMEM] * (1 + len(parts) + (0 if first else 2)),
        out_specs=VMEM if final else (VMEM,) * len(outs),
        scratch_shapes=[pltpu.VMEM((len(pieces), keys, 128), BF)],
        compiler_params=pltpu.CompilerParams(vmem_limit_bytes=24 * 2**20),
        cost_estimate=pl.CostEstimate(
            flops=4 * 2 * rows * len(pieces) * keys * 256,
            transcendentals=2 * rows * len(pieces) * keys,
            bytes_accessed=2**22,
        ),
        name="attention",
    )(queries, *parts, *(held or ()))


def out_kernel(back_ref, tok_ref, weight_ref, out_ref):
    half = back_ref.shape[1]
    low, high = [], []
    mask = lanes_of((half, 128)) < HEAD_DIM
    for pair in range(HEADS // 2):
        even = back_ref[2 * pair].astype(F32)
        odd = back_ref[2 * pair + 1].astype(F32)
        low.append(jnp.where(mask, even, pltpu.roll(odd, HEAD_DIM, 1)).astype(BF))
        high.append(jnp.where(mask, pltpu.roll(even, HEAD_DIM, 1), odd).astype(BF))
    attended = jnp.concatenate(
        [jnp.concatenate(low, axis=1), jnp.concatenate(high, axis=1)], axis=0
    )
    mixed = tok_ref[...] + jnp.dot(attended, weight_ref[...], preferred_element_type=F32)
    cols = out_ref.shape[1]
    rows = out_ref.shape[0]
    columns = [mixed[c * rows : (c + 1) * rows] for c in range(cols)]
    out_ref[...] = jnp.stack(columns, axis=1).astype(BF)


def swaps(offset, count, stride):
    pairs = []
    for i in range(0, count, 2):
        one, two = offset(i) % count, (offset(i) + 1) % count
        for s in range(stride):
            pairs += [(one * stride + s, two * stride + s), (two * stride + s, one * stride + s)]
    return pairs


def body(surface_field, conv_a, conv_b, norm_gain, qkv_weight, out_weight):
    lon_count = lax.axis_size("lon")
    lat_count = lax.axis_size("lat")
    lat = lax.axis_index("lat")
    rows, cols, chans = surface_field.shape
    lon = lax.axis_index("lon")
    even = lon % 2 == 0
    swap = [(c, (c + 1) % lat_count) for c in range(lat_count)]
    first_row = jnp.where(lat == 0, rows - REACH, 0)
    edge = lax.ppermute(
        lax.dynamic_slice_in_dim(surface_field, first_row, REACH, axis=0), "lat", swap
    )

    def columns(at):
        beyond = jnp.concatenate([surface_field[:, at : at + REACH], edge[:, at : at + REACH]])
        return beyond.transpose(1, 0, 2)

    above, below = columns(cols - REACH), columns(0)
    of_pair = lax.ppermute(jnp.where(even, above, below), "lon", swaps(lambda i: i, lon_count, 1))
    of_next = lax.ppermute(
        jnp.where(even, below, above), "lon", swaps(lambda i: i + 1, lon_count, 1)
    )
    field = surface_field.transpose(1, 0, 2)
    edge = edge.transpose(1, 0, 2)

    span = -(-(rows + 4) // 16) * 16
    pooled_cols = cols // 2 + 2
    pooled_rows = rows // 2
    count = (rows // 4) * (cols // 4)
    half = count // 2
    slabs = CB // 128
    where = jnp.stack([lat, jnp.int32(lat_count), lon % 2]).astype(jnp.int32)

    def in_hbm(value):
        return pltpu.with_memory_space_constraint(value, pltpu.HBM)

    weights = (conv_a.reshape(9 * chans, CB), conv_b.reshape(9 * CB, CB), qkv_weight)
    shifted, ready_mid, *here = pl.pallas_call(
        middle_kernel,
        out_shape=(
            jax.ShapeDtypeStruct((3, cols, span, chans), BF),
            jax.ShapeDtypeStruct((3, pooled_cols - 4, pooled_rows, CB), BF),
        )
        + tuple(jax.ShapeDtypeStruct(w.shape, BF) for w in weights),
        in_specs=[SMEM, VMEM, VMEM] + [HBM] * 3,
        out_specs=(VMEM,) * 5,
        scratch_shapes=[
            pltpu.VMEM((cols, span + 8, chans), F32),
            pltpu.VMEM(((pooled_cols - 4) * slabs, span, 128), F32),
            pltpu.SemaphoreType.DMA((3,)),
        ],
        compiler_params=pltpu.CompilerParams(vmem_limit_bytes=24 * 2**20),
        name="middle",
    )(where, field, edge, *[in_hbm(w) for w in weights])
    tokens, outgoing = pl.pallas_call(
        conv_kernel,
        out_shape=(
            jax.ShapeDtypeStruct((count, CB), F32),
            jax.ShapeDtypeStruct((HEADS, count + half, 128), BF),
        ),
        in_specs=[SMEM] + [VMEM] * 8,
        out_specs=(VMEM, VMEM),
        scratch_shapes=[
            pltpu.VMEM((REACH, span + 8, chans), F32),
            pltpu.VMEM((3, REACH, span, chans), BF),
            pltpu.VMEM((3, REACH, span, chans), BF),
            pltpu.VMEM((4 * slabs, span, 128), F32),
            pltpu.VMEM((3, 4, pooled_rows, CB), BF),
            pltpu.VMEM((cols // 4 * slabs, pooled_rows, 128), F32),
        ],
        compiler_params=pltpu.CompilerParams(vmem_limit_bytes=24 * 2**20),
        name="convs",
    )(where, shifted, ready_mid, *here, of_pair, of_next, norm_gain.reshape(1, CB))

    residues = lon_count // HEADS
    groups = [[r * HEADS + h for h in range(HEADS)] for r in range(residues)]
    arrived = lax.all_to_all(outgoing, "lon", 0, 0, axis_index_groups=groups, tiled=True)
    queries = arrived[:, count:].reshape(HEADS * half, 128)
    own = arrived[:, :count].reshape(HEADS * count, 128)

    def other(value):
        return lax.ppermute(value, "lat", swap)

    def pair_swap(value):
        return lax.ppermute(value, "lon", swaps(lambda i: i, residues, HEADS))

    def next_swap(value):
        return lax.ppermute(value, "lon", swaps(lambda i: i + 1, residues, HEADS))

    near = pair_swap(own)
    near_back = next_swap(own)
    queries, *held = attend(queries, [(own,)], None, False)
    own_other = other(own)
    held = attend(queries, [(own_other,)], held, False)
    middle = own.shape[0] // 2
    far_b = next_swap(near[middle:])
    near_other = other(near)
    held = attend(queries, [(near,)], held, False)
    far_a = pair_swap(near_back[:middle])
    near_back_other = other(near_back)
    held = attend(queries, [(near_back,)], held, False)
    held = attend(queries, [(near_other,), (near_back_other,)], held, False)
    far_a_other = other(far_a)
    far_b_other = other(far_b)
    held = attend(queries, [(far_a, far_b)], held, False)
    attended = attend(queries, [(far_a_other, far_b_other)], held, True)
    returned = lax.all_to_all(
        attended.reshape(HEADS, half, 128), "lon", 0, 0, axis_index_groups=groups, tiled=True
    )
    mixed = pl.pallas_call(
        out_kernel,
        out_shape=jax.ShapeDtypeStruct((rows // 4, cols // 4, CB), BF),
        in_specs=[VMEM] * 3,
        out_specs=VMEM,
        compiler_params=pltpu.CompilerParams(vmem_limit_bytes=16 * 2**20),
        name="mix",
    )(returned, tokens, out_weight)
    return mixed


def solution(mesh):
    in_specs = (P(("grp", "lat"), "lon", None), P(), P(), P(), P(), P())
    out_specs = P(("grp", "lat"), "lon", None)
    return jax.shard_map(body, mesh=mesh, in_specs=in_specs, out_specs=out_specs, check_vma=False)
```
